16 devices in a mesh: etp: 2 (over z), ep: 8 (over y, x, core).
Axes of the slice: x: 2, y: 2, z: 2, core: 2. Of those that a mesh axis runs over, the one named last changes fastest.
Arguments:
- hidden: bfloat16 [32768, 1024], P(('ep', 'etp'))
- w_router: float32 [1024, 16], replicated
- expert_ids: int32 [32768, 2], P(('ep', 'etp'))
- d_out: bfloat16 [32768, 1024], P(('ep', 'etp'))
- w_gate: bfloat16 [16, 1024, 3584], P('ep', None, 'etp')
- w_up: bfloat16 [16, 1024, 3584], P('ep', None, 'etp')
- w_down: bfloat16 [16, 3584, 1024], P('ep', 'etp')
Outputs:
- output 1: bfloat16 [32768, 1024], P(('ep', 'etp'))
- output 2: bfloat16 [32768, 1024], P(('ep', 'etp'))
- output 3: float32 [1024, 16], replicated
- output 4: float32 [], replicated
- output 5: float32 [16, 1024, 3584], P('ep', None, 'etp')
- output 6: float32 [16, 1024, 3584], P('ep', None, 'etp')
- output 7: float32 [16, 3584, 1024], P('ep', 'etp')
All inputs are finite; a program needn't handle non-finite values.
Results may differ from the reference program's by a relative error of at most 0.00899328.
Values are sent between devices in bfloat16 or wider.
A program may use at most 1 GiB of HBM per device.

```python
import jax
import jax.numpy as jnp
from jax import lax

EXPERTS = 16
D_MODEL = 1024
D_FF = 3584
TOKENS = 32768
N_DEVICES = 16

CAPACITY = (5 * TOKENS + 2 * EXPERTS - 1) // (2 * EXPERTS)
BLOCK_TOKENS = TOKENS // N_DEVICES


def draw_choices(draw_key):
    quarter = BLOCK_TOKENS // (2 * EXPERTS)
    perm_key, block_key = jax.random.split(draw_key)
    expert_order = jax.random.permutation(perm_key, EXPERTS)
    hot_shift = jnp.zeros((EXPERTS,), jnp.int32).at[:4].set(jnp.array([2, 2, -2, -2], jnp.int32) * quarter)

    def one_block(one_key):
        k_noise, k_rows, k_flip = jax.random.split(one_key, 3)
        count_noise = jax.random.randint(k_noise, (EXPERTS,), 0, quarter + 1)
        count_noise = count_noise.at[0].set(quarter).at[1].set(0)
        count_perm = 4 * quarter + count_noise - jnp.roll(count_noise, -1) + hot_shift
        counts = jnp.zeros((EXPERTS,), jnp.int32).at[expert_order].set(count_perm)
        ends = jnp.cumsum(counts)
        id_seq = jnp.sum(jnp.arange(2 * BLOCK_TOKENS)[:, None] >= ends[None, :], axis=1).astype(jnp.int32)
        id_pairs = jnp.stack([id_seq[:BLOCK_TOKENS], id_seq[BLOCK_TOKENS:]], axis=1)
        id_pairs = id_pairs[jax.random.permutation(k_rows, BLOCK_TOKENS)]
        flip_mask = jax.random.randint(k_flip, (BLOCK_TOKENS, 1), 0, 2) == 1
        return jnp.where(flip_mask, id_pairs[:, ::-1], id_pairs)

    blocks = jax.vmap(one_block)(jax.random.split(block_key, N_DEVICES))
    return blocks.reshape(TOKENS, 2)


def setup_inputs(seed: int = 0) -> dict:
    root_key = jax.random.key(seed)
    k_hid, k_route, k_ids, k_dout, k_gate, k_up, k_down = jax.random.split(root_key, 7)
    hidden = jax.random.normal(k_hid, (TOKENS, D_MODEL), jnp.float32).astype(jnp.bfloat16)
    w_router = jax.random.normal(k_route, (D_MODEL, EXPERTS), jnp.float32) * (0.5 * D_MODEL ** -0.5)
    expert_ids = draw_choices(k_ids)
    d_out = jax.random.normal(k_dout, (TOKENS, D_MODEL), jnp.float32).astype(jnp.bfloat16)
    w_gate = (jax.random.normal(k_gate, (EXPERTS, D_MODEL, D_FF), jnp.float32) * D_MODEL ** -0.5).astype(jnp.bfloat16)
    w_up = (jax.random.normal(k_up, (EXPERTS, D_MODEL, D_FF), jnp.float32) * D_MODEL ** -0.5).astype(jnp.bfloat16)
    w_down = (jax.random.normal(k_down, (EXPERTS, D_FF, D_MODEL), jnp.float32) * D_FF ** -0.5).astype(jnp.bfloat16)
    return {"hidden": hidden, "w_router": w_router, "expert_ids": expert_ids, "d_out": d_out, "w_gate": w_gate, "w_up": w_up, "w_down": w_down}


def route_terms(logits, expert_ids):
    prob_vals = jax.nn.softmax(logits, axis=-1)
    picked = jnp.take_along_axis(prob_vals, expert_ids, axis=1)
    return picked / jnp.sum(picked, axis=1, keepdims=True), jnp.sum(prob_vals, axis=0)


def expert_pass(operands):
    x_buf, dy_buf, gate_w, up_w, down_w = operands
    act_a = jnp.dot(x_buf, gate_w, preferred_element_type=jnp.float32)
    act_b = jnp.dot(x_buf, up_w, preferred_element_type=jnp.float32)
    sig_a = jax.nn.sigmoid(act_a)
    silu_a = act_a * sig_a
    inner_act = (silu_a * act_b).astype(jnp.bfloat16)
    y_buf = jnp.dot(inner_act, down_w, preferred_element_type=jnp.float32).astype(jnp.bfloat16)
    d_inner = jnp.dot(dy_buf, down_w.T, preferred_element_type=jnp.float32)
    d_act_a = (d_inner * act_b * sig_a * (1.0 + act_a * (1.0 - sig_a))).astype(jnp.bfloat16)
    d_act_b = (d_inner * silu_a).astype(jnp.bfloat16)
    dx_buf = (jnp.dot(d_act_a, gate_w.T, preferred_element_type=jnp.float32) + jnp.dot(d_act_b, up_w.T, preferred_element_type=jnp.float32)).astype(jnp.bfloat16)
    g_gate = jnp.dot(x_buf.T, d_act_a, preferred_element_type=jnp.float32)
    g_up = jnp.dot(x_buf.T, d_act_b, preferred_element_type=jnp.float32)
    g_down = jnp.dot(inner_act.T, dy_buf, preferred_element_type=jnp.float32)
    return y_buf, dx_buf, g_gate, g_up, g_down


def reference(hidden, w_router, expert_ids, d_out, w_gate, w_up, w_down):
    hidden_f = hidden.astype(jnp.float32)
    logits = jnp.dot(hidden_f, w_router, preferred_element_type=jnp.float32)
    (gate_vals, prob_sum), route_vjp = jax.vjp(lambda logit_in: route_terms(logit_in, expert_ids), logits)
    n_assign = 2 * TOKENS
    flat_ids = expert_ids.reshape(-1)
    assign = jnp.arange(n_assign, dtype=jnp.int32)
    counts = jnp.bincount(flat_ids, length=EXPERTS)
    sort_order = jnp.argsort(flat_ids * n_assign + assign)
    sort_rank = jnp.zeros((n_assign,), jnp.int32).at[sort_order].set(assign)
    starts = jnp.cumsum(counts) - counts
    slot_pos = sort_rank - starts[flat_ids]
    dest_rows = jnp.where(slot_pos < CAPACITY, flat_ids * CAPACITY + slot_pos, EXPERTS * CAPACITY)
    source = jnp.full((EXPERTS * CAPACITY,), n_assign, jnp.int32).at[dest_rows].set(assign, mode="drop")
    x_buf = jnp.take(hidden, source // 2, axis=0, mode="fill", fill_value=0).reshape(EXPERTS, CAPACITY, D_MODEL)
    d_mix = 2.0 * d_out.astype(jnp.float32)
    dy_assign = (gate_vals[:, :, None] * d_mix[:, None, :]).astype(jnp.bfloat16).reshape(n_assign, D_MODEL)
    dy_buf = jnp.take(dy_assign, source, axis=0, mode="fill", fill_value=0).reshape(EXPERTS, CAPACITY, D_MODEL)
    y_buf, dx_buf, g_gate, g_up, g_down = lax.map(expert_pass, (x_buf, dy_buf, w_gate, w_up, w_down))
    y_pair = jnp.take(y_buf.reshape(EXPERTS * CAPACITY, D_MODEL), dest_rows, axis=0, mode="fill", fill_value=0).reshape(TOKENS, 2, D_MODEL).astype(jnp.float32)
    dx_pair = jnp.take(dx_buf.reshape(EXPERTS * CAPACITY, D_MODEL), dest_rows, axis=0, mode="fill", fill_value=0).reshape(TOKENS, 2, D_MODEL).astype(jnp.float32)
    output = (hidden_f + 2.0 * jnp.sum(gate_vals[:, :, None] * y_pair, axis=1)).astype(jnp.bfloat16)
    d_gates = jnp.sum(d_mix[:, None, :] * y_pair, axis=2)
    route_frac = counts.astype(jnp.float32) / n_assign
    aux_loss = 0.01 * EXPERTS * jnp.sum(route_frac * prob_sum) / TOKENS
    (d_logits,) = route_vjp((d_gates, (0.01 * EXPERTS / TOKENS) * route_frac))
    d_router = jnp.dot(hidden_f.T, d_logits, preferred_element_type=jnp.float32)
    d_hidden = (d_out.astype(jnp.float32) + jnp.sum(dx_pair, axis=1) + jnp.dot(d_logits, w_router.T, preferred_element_type=jnp.float32)).astype(jnp.bfloat16)
    return output, d_hidden, d_router, aux_loss, g_gate, g_up, g_down
```

```python
import functools
import jax
import jax.numpy as jnp
from jax import lax
from jax.experimental import pallas as pl
from jax.experimental.pallas import tpu as pltpu
from jax.sharding import PartitionSpec as P

AUX_COEF = 0.01
OUT_SCALE = 2.0
F32 = jnp.float32
BF16 = jnp.bfloat16
SLOT_TILE = 256
TOK_TILE = 256
TOK_BLOCK = 1024
ROW_TILE = 512
COL = 256
VMEM_LIMIT = 62 * 1024 * 1024

NN = (((1,), (0,)), ((), ()))
NT = (((1,), (1,)), ((), ()))


def dot(lhs, rhs, dims=NN):
    return lax.dot_general(lhs, rhs, dims, preferred_element_type=F32)


def params(n_grid):
    return pltpu.CompilerParams(dimension_semantics=("arbitrary",) * n_grid, vmem_limit_bytes=VMEM_LIMIT)


def dispatch_kernel(scaled, n_tiles, start_ref, slot_ref, gate_ref, rows_ref, out_ref):
    block = pl.program_id(0)
    subs = TOK_BLOCK // TOK_TILE

    @pl.when(block == 0)
    def _():
        out_ref[...] = jnp.zeros_like(out_ref)

    slot_iota = lax.broadcasted_iota(jnp.int32, (SLOT_TILE, TOK_TILE), 0)
    for sub in range(subs):
        cols = slice(sub * TOK_TILE, (sub + 1) * TOK_TILE)
        for e in range(2):
            first = start_ref[e, block * subs + sub]
            last = start_ref[e, block * subs + sub + 1]
            for step in range(2):
                tile = lax.shift_right_logical(first, 8) + step

                @pl.when((tile * SLOT_TILE < last) & (tile < n_tiles) & (first < last))
                def _():
                    base = pl.multiple_of(tile * SLOT_TILE, SLOT_TILE)
                    hit = slot_ref[pl.ds(e, 1), cols] == slot_iota + base
                    acc = dot(hit.astype(F32).astype(BF16), rows_ref[cols, :])
                    if scaled:
                        gate = jnp.sum(jnp.where(hit, gate_ref[pl.ds(e, 1), cols], 0.0), axis=1, keepdims=True)
                        acc = acc * (OUT_SCALE * gate)
                    out_ref[e, pl.ds(base, SLOT_TILE), :] += acc.astype(BF16)


def dispatch(scaled, capacity, starts, slots, gates, rows):
    n_tok, d_model = rows.shape
    return pl.pallas_call(
        functools.partial(dispatch_kernel, scaled, capacity // SLOT_TILE),
        out_shape=jax.ShapeDtypeStruct((2, capacity, d_model), BF16),
        grid_spec=pltpu.PrefetchScalarGridSpec(
            num_scalar_prefetch=1,
            grid=(n_tok // TOK_BLOCK,),
            in_specs=[
                pl.BlockSpec((2, TOK_BLOCK), lambda i, s: (0, i)),
                pl.BlockSpec((2, TOK_BLOCK), lambda i, s: (0, i)),
                pl.BlockSpec((TOK_BLOCK, d_model), lambda i, s: (i, 0)),
            ],
            out_specs=pl.BlockSpec((2, capacity, d_model), lambda i, s: (0, 0, 0)),
        ),
        compiler_params=params(1),
        cost_estimate=pl.CostEstimate(flops=40 * 10**9, bytes_accessed=90 * 10**6, transcendentals=0),
        name="dispatch_c" if scaled else "dispatch_x",
    )(starts, slots, gates, rows)


def forward_kernel(pick_ref, x_ref, wg_ref, wu_ref, u_ref, s_ref, t_ref):
    x = x_ref[0]
    for j in range(wg_ref.shape[2] // COL):
        cols = slice(j * COL, (j + 1) * COL)
        a = dot(x, wg_ref[0, :, cols])
        b = dot(x, wu_ref[0, :, cols])
        sig = jax.nn.sigmoid(a)
        silu = a * sig
        u_ref[0, :, cols] = (silu * b).astype(BF16)
        s_ref[0, :, cols] = silu
        t_ref[0, :, cols] = b * sig * (1.0 + a * (1.0 - sig))


def expert_forward(pick, x_in, w_gate, w_up):
    groups, d_model, width = w_gate.shape
    rows = x_in.shape[1]
    out = lambda dt: jax.ShapeDtypeStruct((groups, rows, width), dt)
    wide = pl.BlockSpec((1, ROW_TILE, width), lambda g, m, s: (g, m, 0))
    weight = pl.BlockSpec((1, d_model, width), lambda g, m, s: (g, 0, 0))
    return pl.pallas_call(
        forward_kernel,
        out_shape=(out(BF16), out(F32), out(F32)),
        grid_spec=pltpu.PrefetchScalarGridSpec(
            num_scalar_prefetch=1,
            grid=(groups, rows // ROW_TILE),
            in_specs=[pl.BlockSpec((1, ROW_TILE, d_model), lambda g, m, s: (s[g], m, 0)), weight, weight],
            out_specs=(wide, wide, wide),
        ),
        compiler_params=params(2),
        cost_estimate=pl.CostEstimate(flops=4 * groups * rows * d_model * width, bytes_accessed=groups * rows * width * 12, transcendentals=groups * rows * width),
        name="expert_forward",
    )(pick, x_in, w_gate, w_up)


def backward_kernel(pick_ref, c_ref, wd_ref, s_ref, t_ref, da_ref, db_ref):
    c = c_ref[0]
    for j in range(wd_ref.shape[1] // COL):
        cols = slice(j * COL, (j + 1) * COL)
        du = dot(c, wd_ref[0, cols, :], NT)
        da_ref[0, :, cols] = (du * t_ref[0, :, cols]).astype(BF16)
        db_ref[0, :, cols] = (du * s_ref[0, :, cols]).astype(BF16)


def expert_backward(pick, c_in, w_down, s_act, t_act):
    groups, width, d_model = w_down.shape
    rows = c_in.shape[1]
    out = jax.ShapeDtypeStruct((groups, rows, width), BF16)
    wide = pl.BlockSpec((1, ROW_TILE, width), lambda g, m, s: (g, m, 0))
    return pl.pallas_call(
        backward_kernel,
        out_shape=(out, out),
        grid_spec=pltpu.PrefetchScalarGridSpec(
            num_scalar_prefetch=1,
            grid=(groups, rows // ROW_TILE),
            in_specs=[
                pl.BlockSpec((1, ROW_TILE, d_model), lambda g, m, s: (s[g], m, 0)),
                pl.BlockSpec((1, width, d_model), lambda g, m, s: (g, 0, 0)),
                wide, wide,
            ],
            out_specs=(wide, wide),
        ),
        compiler_params=params(2),
        cost_estimate=pl.CostEstimate(flops=2 * groups * rows * d_model * width, bytes_accessed=groups * rows * width * 12, transcendentals=0),
        name="expert_backward",
    )(pick, c_in, w_down, s_act, t_act)


def project_kernel(dims, n_terms, pick_ref, *refs):
    lhs, rhs, out_ref = refs[:n_terms], refs[n_terms:-1], refs[-1]
    for j in range(out_ref.shape[1] // COL):
        cols = slice(j * COL, (j + 1) * COL)
        total = None
        for left, right in zip(lhs, rhs):
            weight = right[0, cols, :] if dims is NT else right[0, :, cols]
            term = dot(left[0], weight, dims)
            total = term if total is None else total + term
        out_ref[:, cols] = total.astype(BF16)


def project(dims, own, local_acts, other_acts, local_weights, other_weights):
    acts, weights = list(local_acts) + list(other_acts), list(local_weights) + list(other_weights)
    rows, width = acts[0].shape[1:]
    d_model = weights[0].shape[1] if dims is NT else weights[0].shape[2]
    n_local = len(local_acts)
    act_specs = [pl.BlockSpec((1, ROW_TILE, width), (lambda m, s: (s[0], m, 0)) if i < n_local else (lambda m, s: (0, m, 0))) for i in range(len(acts))]
    weight_specs = [pl.BlockSpec((1,) + weights[i].shape[1:], (lambda m, s: (s[0], 0, 0)) if i < n_local else (lambda m, s: (0, 0, 0))) for i in range(len(weights))]
    return pl.pallas_call(
        functools.partial(project_kernel, dims, len(acts)),
        out_shape=jax.ShapeDtypeStruct((rows, d_model), BF16),
        grid_spec=pltpu.PrefetchScalarGridSpec(
            num_scalar_prefetch=1,
            grid=(rows // ROW_TILE,),
            in_specs=act_specs + weight_specs,
            out_specs=pl.BlockSpec((ROW_TILE, d_model), lambda m, s: (m, 0)),
        ),
        compiler_params=params(1),
        cost_estimate=pl.CostEstimate(flops=2 * len(acts) * rows * d_model * width, bytes_accessed=len(acts) * rows * width * 2, transcendentals=0),
    )(own, *acts, *weights)


def window_kernel(start_ref, rows_ref, out_ref):
    start = pl.multiple_of(start_ref[pl.program_id(0)], 16)
    out_ref[0] = rows_ref[pl.ds(start, out_ref.shape[1]), :]


def cut_windows(starts, rows, window):
    n_win, d_model = starts.shape[0], rows.shape[1]
    return pl.pallas_call(
        window_kernel,
        out_shape=jax.ShapeDtypeStruct((n_win, window, d_model), BF16),
        grid_spec=pltpu.PrefetchScalarGridSpec(
            num_scalar_prefetch=1,
            grid=(n_win,),
            in_specs=[pl.BlockSpec(rows.shape, lambda i, s: (0, 0))],
            out_specs=pl.BlockSpec((1, window, d_model), lambda i, s: (i, 0, 0)),
        ),
        compiler_params=params(1),
        cost_estimate=pl.CostEstimate(flops=10**9, bytes_accessed=25 * 10**6, transcendentals=0),
        name="cut_windows",
    )(starts, rows)


def solution(mesh):
    ep_size = mesh.shape["ep"]
    etp_size = mesh.shape["etp"]
    n_dev = ep_size * etp_size
    all_axes = ("ep", "etp")
    tok_spec = P(all_axes, None)
    gate_spec = P("ep", None, "etp")
    down_spec = P("ep", "etp", None)

    def layer_body(hidden, w_router, expert_ids, d_out, w_gate, w_up, w_down):
        tok_rows, d_model = hidden.shape
        n_experts = w_router.shape[1]
        n_tokens = tok_rows * n_dev
        capacity = (5 * n_tokens + 2 * n_experts - 1) // (2 * n_experts)
        per_expert = 7 * tok_rows // (2 * n_experts)
        window = per_expert + 16
        ep_idx, own = lax.axis_index("ep"), lax.axis_index("etp")
        block_idx = ep_idx * etp_size + own

        x_all = lax.all_gather(hidden, all_axes, tiled=True)
        dy_all = lax.all_gather(d_out, all_axes, tiled=True)

        logits = lax.dot_general(w_router, hidden.astype(F32), (((0,), (1,)), ((), ())), preferred_element_type=F32)
        probs = jax.nn.softmax(logits, axis=0)
        ids = expert_ids.T
        expert_iota = lax.broadcasted_iota(jnp.int32, (n_experts, tok_rows), 0)
        hot0, hot1 = expert_iota == ids[0:1], expert_iota == ids[1:2]
        q0 = jnp.sum(jnp.where(hot0, probs, 0.0), axis=0)
        q1 = jnp.sum(jnp.where(hot1, probs, 0.0), axis=0)
        q_sum = q0 + q1
        g0, g1 = q0 / q_sum, q1 / q_sum

        chosen = (hot0 | hot1).astype(F32)
        pad = lambda v: jnp.pad(v, (0, tok_rows - n_experts))
        payload = jnp.stack([ids[0].astype(F32), ids[1].astype(F32), g0, g1, pad(jnp.sum(chosen, axis=1)), pad(jnp.sum(probs, axis=1))])
        gathered = lax.all_gather(payload, all_axes)
        count_table = gathered[:, 4, :n_experts].astype(jnp.int32)
        prob_sum = jnp.sum(gathered[:, 5, :n_experts], axis=0)
        total_count = jnp.sum(count_table, axis=0)
        prefix_table = jnp.cumsum(count_table, axis=0) - count_table
        window_start = jnp.minimum(prefix_table // 16 * 16, capacity - window)

        mine = (2 * ep_idx + jnp.arange(2, dtype=jnp.int32)).astype(F32)[:, None, None]
        id_first, id_second = gathered[None, :, 0], gathered[None, :, 1]
        is_first, is_second = id_first == mine, id_second == mine
        member = (is_first | is_second).reshape(2, n_tokens // 128, 128)
        gate_in = (jnp.where(is_first, gathered[None, :, 2], 0.0) + jnp.where(is_second, gathered[None, :, 3], 0.0)).reshape(2, n_tokens)
        upper = (lax.broadcasted_iota(jnp.int32, (128, 128), 0) <= lax.broadcasted_iota(jnp.int32, (128, 128), 1)).astype(BF16)
        within = lax.dot_general(member.astype(BF16), upper, (((2,), (0,)), ((), ())), preferred_element_type=F32).astype(jnp.int32)
        row_count = within[:, :, 127]
        row_start = jnp.cumsum(row_count, axis=1) - row_count
        slot = row_start[:, :, None] + within - 1
        slots = jnp.where(member & (slot < capacity), slot, -1).reshape(2, n_tokens)
        sub_start = jnp.concatenate([row_start[:, :: TOK_TILE // 128], (row_start + row_count)[:, -1:]], axis=1)

        pick_pair = jnp.arange(2, dtype=jnp.int32)
        pick_own = own.astype(jnp.int32)[None]
        my_windows = lax.dynamic_index_in_dim(window_start, block_idx, 1, keepdims=False)

        x_in = dispatch(False, capacity, sub_start, slots, gate_in, x_all)
        u_near, s_near, t_near = expert_forward(pick_pair, x_in, w_gate, w_up)

        dy_all, wg_sent, wu_sent, wd_sent = lax.optimization_barrier((dy_all, w_gate, w_up, w_down))
        swap = [(0, 1), (1, 0)]
        send_half = lambda w: lax.ppermute(lax.dynamic_slice_in_dim(w, 1 - own, 1, 0), "etp", swap)
        wg_far, wu_far = send_half(wg_sent), send_half(wu_sent)
        wd_far = send_half(wd_sent)

        dy_all, s_near = lax.optimization_barrier((dy_all, s_near))
        c_in = dispatch(True, capacity, sub_start, slots, gate_in, dy_all)
        da_near, db_near = expert_backward(pick_pair, c_in, w_down, s_near, t_near)
        x_again, da_near, db_near = lax.optimization_barrier((x_in, da_near, db_near))

        def windows_of(rows):
            return cut_windows(my_windows, rows, window)

        def give_back(windows):
            return lax.all_to_all(windows, all_axes, 0, 0, tiled=True).reshape(n_experts * window, d_model)

        u_far, s_far, t_far = expert_forward(pick_own, x_again, wg_far, wu_far)
        y_windows = windows_of(project(NN, pick_own, [u_near], [u_far], [w_down], [wd_far]))
        y_windows, s_far = lax.optimization_barrier((y_windows, s_far))
        y_back = give_back(y_windows)
        da_far, db_far = expert_backward(pick_own, c_in, wd_far, s_far, t_far)
        dx_windows = windows_of(project(NT, pick_own, [da_near, db_near], [da_far, db_far], [w_gate, w_up], [wg_far, wu_far]))
        dx_windows, da_near, db_near, u_near = lax.optimization_barrier((dx_windows, da_near, db_near, u_near))
        dx_back = give_back(dx_windows)

        g_gate = jnp.einsum("erd,erf->edf", x_in, da_near, preferred_element_type=F32)
        g_up = jnp.einsum("erd,erf->edf", x_in, db_near, preferred_element_type=F32)
        g_down = jnp.einsum("erf,erd->efd", u_near, c_in, preferred_element_type=F32)

        local_pos = (jnp.cumsum(chosen, axis=1) - chosen).astype(jnp.int32)
        my_prefix = lax.dynamic_index_in_dim(prefix_table, block_idx, 0, keepdims=False)
        my_start = lax.dynamic_index_in_dim(window_start, block_idx, 0, keepdims=False)
        home_slot = my_prefix[:, None] + local_pos
        home_row = jnp.where(home_slot < capacity, expert_iota * window + home_slot - my_start[:, None], -1)
        row0 = jnp.sum(jnp.where(hot0, home_row, 0), axis=0)
        row1 = jnp.sum(jnp.where(hot1, home_row, 0), axis=0)
        pair_rows = jnp.concatenate([row0, row1])

        def pick_rows(back):
            rows = jnp.take(back, jnp.maximum(pair_rows, 0), axis=0, mode="clip")
            rows = jnp.where((pair_rows >= 0)[:, None], rows.astype(F32), 0.0)
            return rows[:tok_rows], rows[tok_rows:]

        hidden_f = hidden.astype(F32)
        dy_f = d_out.astype(F32)
        y0, y1 = pick_rows(y_back)
        output = (hidden_f + OUT_SCALE * (g0[:, None] * y0 + g1[:, None] * y1)).astype(BF16)
        dg0 = jnp.sum(OUT_SCALE * dy_f * y0, axis=1)
        dg1 = jnp.sum(OUT_SCALE * dy_f * y1, axis=1)

        route_frac = total_count.astype(F32) / (2 * n_tokens)
        aux_loss = AUX_COEF * n_experts * jnp.sum(route_frac * prob_sum) / n_tokens
        mixed = dg0 * g0 + dg1 * g1
        dq0, dq1 = (dg0 - mixed) / q_sum, (dg1 - mixed) / q_sum
        d_prob = jnp.where(hot0, dq0[None], 0.0) + jnp.where(hot1, dq1[None], 0.0) + (AUX_COEF * n_experts / n_tokens) * route_frac[:, None]
        d_logits = probs * (d_prob - jnp.sum(probs * d_prob, axis=0, keepdims=True))
        d_router = lax.dot_general(hidden_f, d_logits, (((0,), (1,)), ((), ())), preferred_element_type=F32)
        d_router = lax.psum(d_router, all_axes)
        dx_back, d_logits = lax.optimization_barrier((dx_back, d_logits))
        dx0, dx1 = pick_rows(dx_back)
        d_hidden = (dy_f + (dx0 + dx1) + lax.dot_general(d_logits, w_router, (((0,), (1,)), ((), ())), preferred_element_type=F32)).astype(BF16)
        return output, d_hidden, d_router, aux_loss, g_gate, g_up, g_down

    return jax.shard_map(layer_body, mesh=mesh, in_specs=(tok_spec, P(), tok_spec, tok_spec, gate_spec, gate_spec, down_spec), out_specs=(tok_spec, tok_spec, P(), P(), gate_spec, gate_spec, down_spec), check_vma=False)
```

```python
import functools
import jax
import jax.numpy as jnp
from jax import lax
from jax.experimental import pallas as pl
from jax.experimental.pallas import tpu as pltpu
from jax.sharding import PartitionSpec as P

AUX_COEF = 0.01
OUT_SCALE = 2.0
F32 = jnp.float32
BF16 = jnp.bfloat16
SLOT_TILE = 256
TOK_TILE = 512
TOK_BLOCK = 1024
ROW_TILE = 512
COL = 256
VMEM_LIMIT = 62 * 1024 * 1024

SEND_ORDER = (13, 9, 1, 15, 11, 3, 12, 8, 14, 10, 5, 7, 4, 6, 2)

NN = (((1,), (0,)), ((), ()))
NT = (((1,), (1,)), ((), ()))


def dot(lhs, rhs, dims=NN):
    return lax.dot_general(lhs, rhs, dims, preferred_element_type=F32)


def params(n_grid):
    return pltpu.CompilerParams(dimension_semantics=("arbitrary",) * n_grid, vmem_limit_bytes=VMEM_LIMIT)


def dispatch_kernel(scaled, n_tiles, start_ref, slot_ref, gate_ref, rows_ref, out_ref):
    block = pl.program_id(0)
    subs = TOK_BLOCK // TOK_TILE

    @pl.when(block == 0)
    def _():
        out_ref[...] = jnp.zeros_like(out_ref)

    slot_iota = lax.broadcasted_iota(jnp.int32, (SLOT_TILE, TOK_TILE), 0)
    for sub in range(subs):
        cols = slice(sub * TOK_TILE, (sub + 1) * TOK_TILE)
        for e in range(2):
            first = start_ref[e, block * subs + sub]
            last = start_ref[e, block * subs + sub + 1]
            for step in range(TOK_TILE // SLOT_TILE + 1):
                tile = lax.shift_right_logical(first, 8) + step

                @pl.when((tile * SLOT_TILE < last) & (tile < n_tiles) & (first < last))
                def _():
                    base = pl.multiple_of(tile * SLOT_TILE, SLOT_TILE)
                    hit = slot_ref[pl.ds(e, 1), cols] == slot_iota + base
                    acc = dot(hit.astype(F32).astype(BF16), rows_ref[cols, :])
                    if scaled:
                        gate = jnp.sum(jnp.where(hit, gate_ref[pl.ds(e, 1), cols], 0.0), axis=1, keepdims=True)
                        acc = acc * (OUT_SCALE * gate)
                    out_ref[e, pl.ds(base, SLOT_TILE), :] += acc.astype(BF16)


def dispatch(scaled, capacity, starts, slots, gates, rows):
    n_tok, d_model = rows.shape
    return pl.pallas_call(
        functools.partial(dispatch_kernel, scaled, capacity // SLOT_TILE),
        out_shape=jax.ShapeDtypeStruct((2, capacity, d_model), BF16),
        grid_spec=pltpu.PrefetchScalarGridSpec(
            num_scalar_prefetch=1,
            grid=(n_tok // TOK_BLOCK,),
            in_specs=[
                pl.BlockSpec((2, TOK_BLOCK), lambda i, s: (0, i)),
                pl.BlockSpec((2, TOK_BLOCK), lambda i, s: (0, i)),
                pl.BlockSpec((TOK_BLOCK, d_model), lambda i, s: (i, 0)),
            ],
            out_specs=pl.BlockSpec((2, capacity, d_model), lambda i, s: (0, 0, 0)),
        ),
        compiler_params=params(1),
        cost_estimate=pl.CostEstimate(flops=40 * 10**9, bytes_accessed=90 * 10**6, transcendentals=0),
        name="dispatch_c" if scaled else "dispatch_x",
    )(starts, slots, gates, rows)


def forward_kernel(pick_ref, x_ref, wg_ref, wu_ref, u_ref, s_ref, t_ref):
    x = x_ref[0]
    for j in range(wg_ref.shape[2] // COL):
        cols = slice(j * COL, (j + 1) * COL)
        a = dot(x, wg_ref[0, :, cols])
        b = dot(x, wu_ref[0, :, cols])
        sig = jax.nn.sigmoid(a)
        silu = a * sig
        u_ref[0, :, cols] = (silu * b).astype(BF16)
        s_ref[0, :, cols] = silu
        t_ref[0, :, cols] = b * sig * (1.0 + a * (1.0 - sig))


def expert_forward(pick, x_in, w_gate, w_up):
    groups, d_model, width = w_gate.shape
    rows = x_in.shape[1]
    out = lambda dt: jax.ShapeDtypeStruct((groups, rows, width), dt)
    wide = pl.BlockSpec((1, ROW_TILE, width), lambda g, m, s: (g, m, 0))
    weight = pl.BlockSpec((1, d_model, width), lambda g, m, s: (g, 0, 0))
    return pl.pallas_call(
        forward_kernel,
        out_shape=(out(BF16), out(F32), out(F32)),
        grid_spec=pltpu.PrefetchScalarGridSpec(
            num_scalar_prefetch=1,
            grid=(groups, rows // ROW_TILE),
            in_specs=[pl.BlockSpec((1, ROW_TILE, d_model), lambda g, m, s: (s[g], m, 0)), weight, weight],
            out_specs=(wide, wide, wide),
        ),
        compiler_params=params(2),
        cost_estimate=pl.CostEstimate(flops=4 * groups * rows * d_model * width, bytes_accessed=groups * rows * width * 12, transcendentals=groups * rows * width),
        name="expert_forward",
    )(pick, x_in, w_gate, w_up)


def backward_kernel(pick_ref, c_ref, wd_ref, s_ref, t_ref, da_ref, db_ref):
    c = c_ref[0]
    for j in range(wd_ref.shape[1] // COL):
        cols = slice(j * COL, (j + 1) * COL)
        du = dot(c, wd_ref[0, cols, :], NT)
        da_ref[0, :, cols] = (du * t_ref[0, :, cols]).astype(BF16)
        db_ref[0, :, cols] = (du * s_ref[0, :, cols]).astype(BF16)


def expert_backward(pick, c_in, w_down, s_act, t_act):
    groups, width, d_model = w_down.shape
    rows = c_in.shape[1]
    out = jax.ShapeDtypeStruct((groups, rows, width), BF16)
    wide = pl.BlockSpec((1, ROW_TILE, width), lambda g, m, s: (g, m, 0))
    return pl.pallas_call(
        backward_kernel,
        out_shape=(out, out),
        grid_spec=pltpu.PrefetchScalarGridSpec(
            num_scalar_prefetch=1,
            grid=(groups, rows // ROW_TILE),
            in_specs=[
                pl.BlockSpec((1, ROW_TILE, d_model), lambda g, m, s: (s[g], m, 0)),
                pl.BlockSpec((1, width, d_model), lambda g, m, s: (g, 0, 0)),
                wide, wide,
            ],
            out_specs=(wide, wide),
        ),
        compiler_params=params(2),
        cost_estimate=pl.CostEstimate(flops=2 * groups * rows * d_model * width, bytes_accessed=groups * rows * width * 12, transcendentals=0),
        name="expert_backward",
    )(pick, c_in, w_down, s_act, t_act)


def project_kernel(dims, n_terms, pick_ref, *refs):
    lhs, rhs, out_ref = refs[:n_terms], refs[n_terms:-1], refs[-1]
    for j in range(out_ref.shape[1] // COL):
        cols = slice(j * COL, (j + 1) * COL)
        total = None
        for left, right in zip(lhs, rhs):
            weight = right[0, cols, :] if dims is NT else right[0, :, cols]
            term = dot(left[0], weight, dims)
            total = term if total is None else total + term
        out_ref[:, cols] = total.astype(BF16)


def project(dims, own, local_acts, other_acts, local_weights, other_weights):
    acts, weights = list(local_acts) + list(other_acts), list(local_weights) + list(other_weights)
    rows, width = acts[0].shape[1:]
    d_model = weights[0].shape[1] if dims is NT else weights[0].shape[2]
    n_local = len(local_acts)
    act_specs = [pl.BlockSpec((1, ROW_TILE, width), (lambda m, s: (s[0], m, 0)) if i < n_local else (lambda m, s: (0, m, 0))) for i in range(len(acts))]
    weight_specs = [pl.BlockSpec((1,) + weights[i].shape[1:], (lambda m, s: (s[0], 0, 0)) if i < n_local else (lambda m, s: (0, 0, 0))) for i in range(len(weights))]
    return pl.pallas_call(
        functools.partial(project_kernel, dims, len(acts)),
        out_shape=jax.ShapeDtypeStruct((rows, d_model), BF16),
        grid_spec=pltpu.PrefetchScalarGridSpec(
            num_scalar_prefetch=1,
            grid=(rows // ROW_TILE,),
            in_specs=act_specs + weight_specs,
            out_specs=pl.BlockSpec((ROW_TILE, d_model), lambda m, s: (m, 0)),
        ),
        compiler_params=params(1),
        cost_estimate=pl.CostEstimate(flops=2 * len(acts) * rows * d_model * width, bytes_accessed=len(acts) * rows * width * 2, transcendentals=0),
    )(own, *acts, *weights)


def window_kernel(start_ref, rows_ref, *out_refs):
    for i, out_ref in enumerate(out_refs):
        start = pl.multiple_of(start_ref[i], 16)
        out_ref[...] = rows_ref[pl.ds(start, out_ref.shape[0]), :]


def cut_windows(starts, rows, window):
    n_win, (n_rows, d_model) = starts.shape[0], rows.shape
    return pl.pallas_call(
        window_kernel,
        out_shape=(jax.ShapeDtypeStruct((window, d_model), BF16),) * n_win,
        grid_spec=pltpu.PrefetchScalarGridSpec(
            num_scalar_prefetch=1,
            grid=(d_model // COL,),
            in_specs=[pl.BlockSpec((n_rows, COL), lambda i, s: (0, i))],
            out_specs=(pl.BlockSpec((window, COL), lambda i, s: (0, i)),) * n_win,
        ),
        compiler_params=params(1),
        cost_estimate=pl.CostEstimate(flops=10**9, bytes_accessed=25 * 10**6, transcendentals=0),
        name="cut_windows",
    )(starts, rows)


def join_kernel(*refs):
    blocks, out_ref = refs[:-1], refs[-1]
    window = blocks[0].shape[0]
    for i, block in enumerate(blocks):
        out_ref[i * window : (i + 1) * window, :] = block[...]


def join_windows(blocks):
    n_win, (window, d_model) = len(blocks), blocks[0].shape
    return pl.pallas_call(
        join_kernel,
        out_shape=jax.ShapeDtypeStruct((n_win * window, d_model), BF16),
        grid=(d_model // COL,),
        in_specs=[pl.BlockSpec((window, COL), lambda i: (0, i))] * n_win,
        out_specs=pl.BlockSpec((n_win * window, COL), lambda i: (0, i)),
        compiler_params=params(1),
        cost_estimate=pl.CostEstimate(flops=10**9, bytes_accessed=30 * 10**6, transcendentals=0),
        name="join_windows",
    )(*blocks)


def solution(mesh):
    ep_size = mesh.shape["ep"]
    etp_size = mesh.shape["etp"]
    n_dev = ep_size * etp_size
    all_axes = ("ep", "etp")
    tok_spec = P(all_axes, None)
    gate_spec = P("ep", None, "etp")
    down_spec = P("ep", "etp", None)

    def layer_body(hidden, w_router, expert_ids, d_out, w_gate, w_up, w_down):
        tok_rows, _ = hidden.shape
        n_experts = w_router.shape[1]
        n_tokens = tok_rows * n_dev
        capacity = (5 * n_tokens + 2 * n_experts - 1) // (2 * n_experts)
        per_expert = 7 * tok_rows // (2 * n_experts)
        window = per_expert + 16
        ep_idx, own = lax.axis_index("ep"), lax.axis_index("etp")
        block_idx = ep_idx * etp_size + own

        x_all = lax.all_gather(hidden, all_axes, tiled=True)
        dy_all = lax.all_gather(d_out, all_axes, tiled=True)

        logits = lax.dot_general(w_router, hidden.astype(F32), (((0,), (1,)), ((), ())), preferred_element_type=F32)
        probs = jax.nn.softmax(logits, axis=0)
        ids = expert_ids.T
        expert_iota = lax.broadcasted_iota(jnp.int32, (n_experts, tok_rows), 0)
        hot0, hot1 = expert_iota == ids[0:1], expert_iota == ids[1:2]
        q0 = jnp.sum(jnp.where(hot0, probs, 0.0), axis=0)
        q1 = jnp.sum(jnp.where(hot1, probs, 0.0), axis=0)
        q_sum = q0 + q1
        g0, g1 = q0 / q_sum, q1 / q_sum

        chosen = (hot0 | hot1).astype(F32)
        pad = lambda v: jnp.pad(v, (0, tok_rows - n_experts))
        payload = jnp.stack([ids[0].astype(F32), ids[1].astype(F32), g0, g1, pad(jnp.sum(chosen, axis=1)), pad(jnp.sum(probs, axis=1))])
        gathered = lax.all_gather(payload, all_axes)
        count_table = gathered[:, 4, :n_experts].astype(jnp.int32)
        prob_sum = jnp.sum(gathered[:, 5, :n_experts], axis=0)
        total_count = jnp.sum(count_table, axis=0)
        prefix_table = jnp.cumsum(count_table, axis=0) - count_table
        window_start = jnp.minimum(prefix_table // 16 * 16, capacity - window)

        mine = (2 * ep_idx + jnp.arange(2, dtype=jnp.int32)).astype(F32)[:, None, None]
        id_first, id_second = gathered[None, :, 0], gathered[None, :, 1]
        is_first, is_second = id_first == mine, id_second == mine
        member = (is_first | is_second).reshape(2, n_tokens // 128, 128)
        gate_in = (jnp.where(is_first, gathered[None, :, 2], 0.0) + jnp.where(is_second, gathered[None, :, 3], 0.0)).reshape(2, n_tokens)
        upper = (lax.broadcasted_iota(jnp.int32, (128, 128), 0) <= lax.broadcasted_iota(jnp.int32, (128, 128), 1)).astype(BF16)
        within = lax.dot_general(member.astype(BF16), upper, (((2,), (0,)), ((), ())), preferred_element_type=F32).astype(jnp.int32)
        row_count = within[:, :, 127]
        row_start = jnp.cumsum(row_count, axis=1) - row_count
        slot = row_start[:, :, None] + within - 1
        slots = jnp.where(member & (slot < capacity), slot, -1).reshape(2, n_tokens)
        sub_start = jnp.concatenate([row_start[:, :: TOK_TILE // 128], (row_start + row_count)[:, -1:]], axis=1)

        pick_pair = jnp.arange(2, dtype=jnp.int32)
        pick_own = own.astype(jnp.int32)[None]
        partner = jnp.arange(n_dev, dtype=jnp.int32) ^ block_idx
        my_windows = jnp.take(lax.dynamic_index_in_dim(window_start, block_idx, 1, keepdims=False), partner)

        x_in = dispatch(False, capacity, sub_start, slots, gate_in, x_all)
        u_near, s_near, t_near = expert_forward(pick_pair, x_in, w_gate, w_up)

        half_of = lambda w: lax.dynamic_slice_in_dim(w, 1 - own, 1, 0)
        wg_sent, wu_sent, wd_sent = lax.optimization_barrier((half_of(w_gate), half_of(w_up), half_of(w_down)))
        dy_all, wg_sent, wu_sent, wd_sent = lax.optimization_barrier((dy_all, wg_sent, wu_sent, wd_sent))
        swap = [(0, 1), (1, 0)]
        send_half = lambda w: lax.ppermute(w, "etp", swap)
        wg_far, wu_far = send_half(wg_sent), send_half(wu_sent)
        wd_far = send_half(wd_sent)

        dy_all, s_near = lax.optimization_barrier((dy_all, s_near))
        c_in = dispatch(True, capacity, sub_start, slots, gate_in, dy_all)
        da_near, db_near = expert_backward(pick_pair, c_in, w_down, s_near, t_near)
        x_again, da_near, db_near = lax.optimization_barrier((x_in, da_near, db_near))

        def windows_of(rows):
            return cut_windows(my_windows, rows, window)

        def give_back(windows):
            place = lambda b: (b % etp_size) * ep_size + b // etp_size
            blocks = list(windows)
            for i in SEND_ORDER:
                blocks[i] = lax.ppermute(windows[i], ("etp", "ep"), [(place(b), place(b ^ i)) for b in range(n_dev)])
            return blocks

        u_far, s_far, t_far = expert_forward(pick_own, x_again, wg_far, wu_far)
        y_windows = windows_of(project(NN, pick_own, [u_near], [u_far], [w_down], [wd_far]))
        y_windows, s_far = lax.optimization_barrier((y_windows, s_far))
        y_blocks = give_back(y_windows)
        y_back = join_windows(y_blocks)
        da_far, db_far = expert_backward(pick_own, c_in, wd_far, s_far, t_far)
        dx_windows = windows_of(project(NT, pick_own, [da_near, db_near], [da_far, db_far], [w_gate, w_up], [wg_far, wu_far]))
        dx_windows, da_near, db_near, u_near = lax.optimization_barrier((dx_windows, da_near, db_near, u_near))
        dx_blocks = give_back(dx_windows)
        dx_back = join_windows(dx_blocks)

        g_gate = jnp.einsum("erd,erf->edf", x_in, da_near, preferred_element_type=F32)
        g_up = jnp.einsum("erd,erf->edf", x_in, db_near, preferred_element_type=F32)
        local_pos = (jnp.cumsum(chosen, axis=1) - chosen).astype(jnp.int32)
        my_prefix = lax.dynamic_index_in_dim(prefix_table, block_idx, 0, keepdims=False)
        my_start = lax.dynamic_index_in_dim(window_start, block_idx, 0, keepdims=False)
        home_slot = my_prefix[:, None] + local_pos
        home_row = jnp.where(home_slot < capacity, (expert_iota ^ block_idx) * window + home_slot - my_start[:, None], -1)
        row0 = jnp.sum(jnp.where(hot0, home_row, 0), axis=0)
        row1 = jnp.sum(jnp.where(hot1, home_row, 0), axis=0)
        pair_rows = jnp.concatenate([row0, row1])

        def pick_rows(back):
            rows = jnp.take(back, jnp.maximum(pair_rows, 0), axis=0, mode="clip")
            rows = jnp.where((pair_rows >= 0)[:, None], rows.astype(F32), 0.0)
            return rows[:tok_rows], rows[tok_rows:]

        hidden_f = hidden.astype(F32)
        dy_f = d_out.astype(F32)
        y0, y1 = pick_rows(y_back)
        output = (hidden_f + OUT_SCALE * (g0[:, None] * y0 + g1[:, None] * y1)).astype(BF16)
        dg0 = jnp.sum(OUT_SCALE * dy_f * y0, axis=1)
        dg1 = jnp.sum(OUT_SCALE * dy_f * y1, axis=1)

        route_frac = total_count.astype(F32) / (2 * n_tokens)
        aux_loss = AUX_COEF * n_experts * jnp.sum(route_frac * prob_sum) / n_tokens
        mixed = dg0 * g0 + dg1 * g1
        dq0, dq1 = (dg0 - mixed) / q_sum, (dg1 - mixed) / q_sum
        d_prob = jnp.where(hot0, dq0[None], 0.0) + jnp.where(hot1, dq1[None], 0.0) + (AUX_COEF * n_experts / n_tokens) * route_frac[:, None]
        d_logits = probs * (d_prob - jnp.sum(probs * d_prob, axis=0, keepdims=True))
        d_router = lax.dot_general(hidden_f, d_logits, (((0,), (1,)), ((), ())), preferred_element_type=F32)
        u_near, d_router = lax.optimization_barrier((u_near, d_router))
        d_router = lax.psum(d_router, all_axes)
        g_down = jnp.einsum("erf,erd->efd", u_near, c_in, preferred_element_type=F32)
        dx_back, d_logits = lax.optimization_barrier((dx_back, d_logits))
        dx0, dx1 = pick_rows(dx_back)
        d_hidden = (dy_f + (dx0 + dx1) + lax.dot_general(d_logits, w_router, (((0,), (1,)), ((), ())), preferred_element_type=F32)).astype(BF16)
        return output, d_hidden, d_router, aux_loss, g_gate, g_up, g_down

    return jax.shard_map(layer_body, mesh=mesh, in_specs=(tok_spec, P(), tok_spec, tok_spec, gate_spec, gate_spec, down_spec), out_specs=(tok_spec, tok_spec, P(), P(), gate_spec, gate_spec, down_spec), check_vma=False)
```
